32 devices in a mesh: rep: 4 (over x, y), dp: 8 (over z, core).
Axes of the slice: x: 2, y: 2, z: 4, core: 2. Of those that a mesh axis runs over, the one named last changes fastest.
Arguments:
- x: bfloat16 [32, 2048, 768], P(('rep', 'dp')), parts along dimension 0
- dy: bfloat16 [32, 2048, 768], P(('rep', 'dp')), parts along dimension 0
- w_gate: bfloat16 [2, 768, 4480], replicated
- w_up: bfloat16 [2, 768, 4480], replicated
- w_down: bfloat16 [2, 4480, 768], replicated
- m_w_gate: float32 [2, 768, 4480], P(None, 'dp')
- m_w_up: float32 [2, 768, 4480], P(None, 'dp')
- m_w_down: float32 [2, 4480, 768], P(None, 'dp')
- v_w_gate: float32 [2, 768, 4480], P(None, 'dp')
- v_w_up: float32 [2, 768, 4480], P(None, 'dp')
- v_w_down: float32 [2, 4480, 768], P(None, 'dp')
Outputs:
- output 1: bfloat16 [8, 768, 4480], P('rep'), parts along dimension 0
- output 2: bfloat16 [8, 768, 4480], P('rep'), parts along dimension 0
- output 3: bfloat16 [8, 4480, 768], P('rep'), parts along dimension 0
- output 4: float32 [8, 768, 4480], P('rep', 'dp'), parts along dimension 0
- output 5: float32 [8, 768, 4480], P('rep', 'dp'), parts along dimension 0
- output 6: float32 [8, 4480, 768], P('rep', 'dp'), parts along dimension 0
- output 7: float32 [8, 768, 4480], P('rep', 'dp'), parts along dimension 0
- output 8: float32 [8, 768, 4480], P('rep', 'dp'), parts along dimension 0
- output 9: float32 [8, 4480, 768], P('rep', 'dp'), parts along dimension 0
There are 4 independent parts. The reference program is written for one: setup_inputs(seed, part) draws one part's arguments, and reference() takes and returns one part's arrays. A program takes and returns all parts, laid end to end along the dimension named above; an argument that names none is the same for every part.
All inputs are finite; a program needn't handle non-finite values.
Results may differ from the reference program's by a relative error of at most 0.022.
Values are sent between devices in bfloat16 or wider.
A program may use at most 2 GiB of HBM per device.

```python
import jax
import jax.numpy as jnp
from jax import lax

SEQUENCES = 8
TOKENS = 2048
D = 768
FF = 4480
LAYERS = 2
NAMES = ("w_gate", "w_up", "w_down")
SHAPES = {"w_gate": (LAYERS, D, FF), "w_up": (LAYERS, D, FF), "w_down": (LAYERS, FF, D)}


def bump(key, n, height):
    away = (jnp.arange(n, dtype=jnp.int32) - jax.random.randint(key, (), 0, n, jnp.int32)) % n
    return jnp.where(away < n // 8, height, 1.0)


def together(key, own, strength):
    shared = jax.random.normal(key, own.shape[1:], jnp.float32)
    return (own + strength * shared) * lax.rsqrt(1 + strength * strength)


def setup_inputs(seed: int = 0, part: int = 0) -> dict:
    kx, kdy, ka, kb, kz, kf, kh, kl, *keys = jax.random.split(jax.random.key(seed), 8 + 3 * len(NAMES))
    kx, kdy, ka, kb = (jax.random.fold_in(k, part) for k in (kx, kdy, ka, kb))
    kw, km, kv = (keys[i::3] for i in range(3))
    shape = (SEQUENCES, TOKENS, D)
    much_x, much_dy = jax.random.uniform(kz, (2,), jnp.float32, 0.0, 1.0)
    loud = 2.0 ** jax.random.uniform(jax.random.fold_in(kz, 1), (), jnp.float32, -1.0, 2.0)
    layers = 2.0 ** jax.random.uniform(kl, (LAYERS, 1, 1), jnp.float32, -1.0, 1.0)
    x = together(ka, jax.random.normal(kx, shape, jnp.float32), much_x) * bump(kf, D, 4.0)
    dy = together(kb, jax.random.normal(kdy, shape, jnp.float32), much_dy)
    drawn = {"x": x.astype(jnp.bfloat16), "dy": (loud * dy * (SEQUENCES * TOKENS) ** -0.5).astype(jnp.bfloat16)}
    for key, name in zip(kw, NAMES, strict=True):
        w = jax.random.normal(key, SHAPES[name], jnp.float32) * SHAPES[name][1] ** -0.5
        drawn[name] = (w * {"w_gate": 1.0, "w_up": bump(kh, FF, 4.0), "w_down": layers}[name]).astype(jnp.bfloat16)
    for key, name in zip(km, NAMES, strict=True):
        drawn[f"m_{name}"] = 0.1 * jax.random.normal(key, SHAPES[name], jnp.float32)
    for key, name in zip(kv, NAMES, strict=True):
        drawn[f"v_{name}"] = jax.random.uniform(key, SHAPES[name], jnp.float32, 0.005, 0.015)
    return drawn


def matmul(a, w):
    return jnp.dot(a, w, preferred_element_type=jnp.float32).astype(jnp.bfloat16)


def normed(h):
    wide = h.astype(jnp.float32)
    scale = lax.rsqrt(jnp.mean(wide**2, -1, keepdims=True) + 1e-6)
    return (wide * scale).astype(jnp.bfloat16)


def layer(h, w):
    a = normed(h)
    gate = jnp.dot(a, w["w_gate"], preferred_element_type=jnp.float32)
    up = jnp.dot(a, w["w_up"], preferred_element_type=jnp.float32)
    return h + matmul((jax.nn.silu(gate) * up).astype(jnp.bfloat16), w["w_down"])


def adamw(w, m, v, g):
    m = 0.9 * m + 0.1 * g
    v = 0.95 * v + 0.05 * g * g
    step = m * lax.rsqrt(v + 1e-8) + 0.1 * w
    return (w - 0.02 * step).astype(jnp.bfloat16), m, v


def clipped(gradients, sum_of_squares, count):
    factor = jnp.minimum(1.0, 0.5 * lax.rsqrt(sum_of_squares / count + 1e-30))
    return [g * factor for g in gradients]


def stack(weights, h):
    return lax.scan(lambda h, w: (layer(h, w), None), h, weights)[0]


def reference(x, dy, w_gate, w_up, w_down, m_w_gate, m_w_up, m_w_down, v_w_gate, v_w_up, v_w_down):
    weights = dict(zip(NAMES, (w_gate, w_up, w_down), strict=True))

    def take(so_far, sequence):
        h, by_y = sequence
        _, back = jax.vjp(lambda w: stack(w, h), weights)
        return jax.tree.map(lambda total, term: total + term.astype(jnp.float32), so_far, back(by_y)[0]), None

    none_yet = {name: jnp.zeros(w.shape, jnp.float32) for name, w in weights.items()}
    by_weights, _ = lax.scan(take, none_yet, (x, dy))
    gradients = [by_weights[name].astype(jnp.bfloat16).astype(jnp.float32) for name in NAMES]
    gradients = clipped(gradients, sum(jnp.sum(g * g) for g in gradients), sum(g.size for g in gradients))
    new = [
        adamw(w.astype(jnp.float32), m, v, g)
        for w, m, v, g in zip((w_gate, w_up, w_down), (m_w_gate, m_w_up, m_w_down), (v_w_gate, v_w_up, v_w_down), gradients, strict=True)
    ]
    return tuple(one[which] for which in range(3) for one in new)
```

```python
import functools

import jax
import jax.numpy as jnp
from jax import lax
from jax.experimental import pallas as pl
from jax.experimental.pallas import tpu as pltpu
from jax.sharding import PartitionSpec as P

MESH = pl.DeviceIdType.MESH
f32, bf16 = jnp.float32, jnp.bfloat16
T, D, F = 2048, 768, 4480
BF = 640
NB = F // BF
TC = 512
HD = 384
HB = 320
GRP, DOWN = 96, 560


def sig(x):
    return 0.5 * jnp.tanh(0.5 * x) + 0.5

def ka_kernel(x_ref, wg_ref, wu_ref, wd_ref, h_ref, a_s, w_s, wd_s, hid_s, sems, wd_sem, *, layer):
    def fetch(j):
        s = j % 2
        c = pl.ds(pl.multiple_of(j * BF, 128), BF)
        return (pltpu.make_async_copy(wg_ref.at[layer, :, c], w_s.at[s, :, pl.ds(0, BF)], sems.at[s, 0]),
                pltpu.make_async_copy(wu_ref.at[layer, :, c], w_s.at[s, :, pl.ds(BF, BF)], sems.at[s, 1]))
    for c in fetch(0): c.start()
    wdc = pltpu.make_async_copy(wd_ref.at[layer], wd_s, wd_sem)
    def norm(r, _):
        rows = pl.ds(pl.multiple_of(r * TC, TC), TC)
        wide = x_ref[rows, :].astype(jnp.float32)
        scale = lax.rsqrt(jnp.mean(wide * wide, -1, keepdims=True) + 1e-6)
        a_s[rows, :] = (wide * scale).astype(jnp.bfloat16)
        return _
    lax.fori_loop(0, T // TC, norm, 0)
    def block(j, z):
        s = lax.rem(j, 2)
        @pl.when(j + 1 < NB)
        def _():
            for c in fetch(j + 1): c.start()
        @pl.when(j == 0)
        def _(): wdc.start()
        for c in fetch(j): c.wait()
        def rowsf(r, _):
            rows = pl.ds(pl.multiple_of(r * TC, TC), TC)
            gu = jnp.dot(a_s[rows, :], w_s[s], preferred_element_type=jnp.float32)
            gate, up = gu[:, :BF], gu[:, BF:]
            hid_s[rows, pl.ds(pl.multiple_of(j * BF, 128), BF)] = (gate * sig(gate) * up).astype(jnp.bfloat16)
            return _
        lax.fori_loop(0, T // TC, rowsf, 0)
        return z
    lax.fori_loop(0, NB, block, 0)
    wdc.wait()
    def down(r, _):
        rows = pl.ds(pl.multiple_of(r * TC, TC), TC)
        y = jnp.dot(hid_s[rows, :], wd_s[...], preferred_element_type=jnp.float32).astype(jnp.bfloat16)
        h_ref[rows, :] = x_ref[rows, :] + y
        return _
    lax.fori_loop(0, T // TC, down, 0)

def ka(x, wg, wu, wd, layer=0):
    V = pl.BlockSpec(memory_space=pltpu.VMEM); A = pl.BlockSpec(memory_space=pl.ANY)
    return pl.pallas_call(functools.partial(ka_kernel, layer=layer), out_shape=jax.ShapeDtypeStruct((T, D), jnp.bfloat16),
        in_specs=[V, A, A, A], out_specs=V,
        scratch_shapes=[pltpu.VMEM((T, D), jnp.bfloat16), pltpu.VMEM((2, D, 2 * BF), jnp.bfloat16), pltpu.VMEM((F, D), jnp.bfloat16),
                        pltpu.VMEM((T, F), jnp.bfloat16), pltpu.SemaphoreType.DMA((2, 2)), pltpu.SemaphoreType.DMA],
        compiler_params=pltpu.CompilerParams(vmem_limit_bytes=60 << 20), name="ka")(x, wg, wu, wd)


RING = 4


def block_of(i):
    return jnp.where(i % 2 == 0, i // 2, NB - 1 - i // 2)

def lkernel(h_ref, dh_ref, wg_ref, wu_ref, wd_ref, *rest, layer, with_da, comm):
    if with_da:
        dho_ref, *rest = rest
    (guf_ref, df_ref, ss_ref, a_s, w_s, wd_s, hid_s, dgu_s, bgu, bd, sgu, sd, igu, idd, ss_s, *rest) = rest
    if with_da:
        da_s, *rest = rest
    (wsem, rgu, rd, sendgu, sendd, d2dgu_s, d2dd_s, d2dgu_r, d2dd_r, fsem_gu, fsem_d, cred) = rest
    me = lax.axis_index("dp")
    chip = me // 2
    core = me % 2
    sib = me + 1 - 2 * core
    pos = (3 - chip, chip)
    nxt = (me - 2, me + 2)

    def rdma(src, dst, ssem, rsem, dev):
        return pltpu.make_async_remote_copy(src, dst, ssem, rsem, device_id={"dp": dev}, device_id_type=MESH)

    if comm:
        bar = pltpu.get_barrier_semaphore()
        pl.semaphore_signal(bar, inc=1, device_id={"dp": sib}, device_id_type=MESH)
        @pl.when(chip > 0)
        def _(): pl.semaphore_signal(bar, inc=1, device_id={"dp": me - 2}, device_id_type=MESH)
        @pl.when(chip < 3)
        def _(): pl.semaphore_signal(bar, inc=1, device_id={"dp": me + 2}, device_id_type=MESH)

    def fetch(i):
        s = i % 2
        b = block_of(i)
        c = pl.ds(pl.multiple_of(b * BF, 128), BF)
        return (pltpu.make_async_copy(wg_ref.at[layer, :, c], w_s.at[s, :, pl.ds(0, BF)], wsem.at[s, 0]),
                pltpu.make_async_copy(wu_ref.at[layer, :, c], w_s.at[s, :, pl.ds(BF, BF)], wsem.at[s, 1]),
                pltpu.make_async_copy(wd_ref.at[layer, c, :], wd_s.at[s], wsem.at[s, 2]))
    for c in fetch(0): c.start()

    def norm(r, z):
        rows = pl.ds(pl.multiple_of(r * TC, TC), TC)
        wide = h_ref[rows, :].astype(f32)
        scale = lax.rsqrt(jnp.mean(wide * wide, -1, keepdims=True) + 1e-6)
        a_s[rows, :] = (wide * scale).astype(bf16)
        if with_da:
            da_s[rows, :] = jnp.zeros((TC, D), f32)
        return z
    lax.fori_loop(0, T // TC, norm, 0)
    ss_s[...] = jnp.zeros_like(ss_s)
    if comm:
        pl.semaphore_wait(bar, 1 + (chip > 0).astype(jnp.int32) + (chip < 3).astype(jnp.int32))

    def d2d_gu(i):
        return rdma(bgu.at[RING], sgu.at[i % RING], d2dgu_s, d2dgu_r.at[i % RING], sib)
    def d2d_d(i):
        return rdma(bd.at[RING], sd.at[i % RING], d2dd_s, d2dd_r.at[i % RING], sib)
    def msg_gu(i, d):
        return rdma(bgu.at[i % RING, pl.ds(2 * d, 2)], igu.at[d, i], sendgu.at[i % RING, d], rgu.at[d, i], nxt[d])
    def msg_d(i, h, d):
        return rdma(bd.at[i % RING, h], idd.at[i, h], sendd.at[i % RING, h], rd.at[i, h], nxt[d])
    def fin_gu(i, d):
        return pltpu.make_async_copy(bgu.at[i % RING, pl.ds(2 * d, 2)], guf_ref.at[block_of(i)], fsem_gu.at[i % RING])
    def fin_d(i, h, d):
        return pltpu.make_async_copy(bd.at[i % RING, h], df_ref.at[2 * block_of(i) + h - (NB if d else 0)], fsem_d.at[i % RING, h])

    def add(own, sibv, inc, n, width, p):
        def go(r, z, first, last):
            rows = pl.ds(pl.multiple_of(r * 32, 32), 32)
            total = own[rows, :].astype(f32) + sibv[rows, :].astype(f32)
            if not first:
                total = total + inc[rows, :].astype(f32)
            out = total.astype(bf16)
            own[rows, :] = out
            if last:
                sq = out.astype(f32)
                ss_s[:, :width] += sq * sq
            return z
        for first, last, cond in ((True, False, p == 0), (False, False, (p > 0) & (p < 3)), (False, True, p == 3)):
            @pl.when(cond)
            def _(): lax.fori_loop(0, n // 32, functools.partial(go, first=first, last=last), 0)

    def process_gu(s):
        for d in (0, 1):
            p = pos[d]
            i = s - 1 - p
            @pl.when((i >= 0) & (i < NB))
            def _():
                if d == 0:
                    pass
                @pl.when(p > 0)
                def _(): msg_gu(i, d).wait_recv()
                for k in (0, 1):
                    add(bgu.at[i % RING, 2 * d + k], sgu.at[i % RING, 2 * d + k], igu.at[d, i, k], GRP, 2 * BF, p)
                @pl.when(p < 3)
                def _(): msg_gu(i, d).start()
                @pl.when(p == 3)
                def _(): fin_gu(i, d).start()

    def process_d(s):
        for d in (0, 1):
            p = pos[d]
            i = s - p
            for h in (0, 1):
                mine = jnp.where(i == NB - 1, h == d, i % 2 == d)
                @pl.when((i >= 0) & (i < NB) & mine)
                def _():
                    @pl.when(p > 0)
                    def _(): msg_d(i, h, d).wait_recv()
                    add(bd.at[i % RING, h], sd.at[i % RING, h], idd.at[i, h], HB, HD, p)
                    @pl.when(p < 3)
                    def _(): msg_d(i, h, d).start()
                    @pl.when(p == 3)
                    def _(): fin_d(i, h, d).start()

    def settle_gu(i):
        for d in (0, 1):
            @pl.when(pos[d] < 3)
            def _(): msg_gu(i, d).wait_send()
            @pl.when(pos[d] == 3)
            def _(): fin_gu(i, d).wait()
    def settle_d(i):
        for d in (0, 1):
            for h in (0, 1):
                mine = jnp.where(i == NB - 1, h == d, i % 2 == d)
                @pl.when(mine & (pos[d] < 3))
                def _(): msg_d(i, h, d).wait_send()
                @pl.when(mine & (pos[d] == 3))
                def _(): fin_d(i, h, d).wait()

    def wait_sib_gu(i):
        @pl.when((i >= 0) & (i < NB))
        def _(): d2d_gu(i).wait_recv()
    def wait_sib_d(i):
        @pl.when((i >= 0) & (i < NB))
        def _(): d2d_d(i).wait_recv()

    def step(s, z):
        w = lax.rem(s, 2)
        @pl.when(s < NB)
        def _():
            @pl.when(s + 1 < NB)
            def _():
                for c in fetch(s + 1): c.start()
            for c in fetch(s): c.wait()
            def ff(r, zz):
                rows = pl.ds(pl.multiple_of(r * TC, TC), TC)
                gu = jnp.dot(a_s[rows, :], w_s[w], preferred_element_type=f32)
                dhid = lax.dot_general(dh_ref[rows, :], wd_s[w], (((1,), (1,)), ((), ())), preferred_element_type=f32).astype(bf16).astype(f32)
                gate, up = gu[:, :BF], gu[:, BF:]
                sg = sig(gate)
                silu = gate * sg
                hid_s[rows, :] = (silu * up).astype(bf16)
                dgu_s[rows, BF:] = (dhid * silu).astype(bf16)
                dgu_s[rows, :BF] = (dhid * up * (sg + silu * (1.0 - sg))).astype(bf16)
                return zz
            lax.fori_loop(0, T // TC, ff, 0)
            if comm:
                @pl.when(s >= RING)
                def _(): settle_d(s - RING)
                @pl.when(s >= 1)
                def _(): d2d_d(s - 1).wait_send()
            g = lax.dot_general(hid_s[...], dh_ref[...], (((0,), (0,)), ((), ())), preferred_element_type=f32).astype(bf16)
            for q in (0, 1):
                idx = jnp.where(core == q, s % RING, RING)
                for h in (0, 1):
                    bd[idx, h] = g[HB * h:HB * (h + 1), HD * q:HD * (q + 1)]
            if comm:
                @pl.when(s >= RING)
                def _(): pl.semaphore_wait(cred.at[0], 1)
                d2d_d(s).start()
        if comm:
            wait_sib_gu(s - 1)
            process_gu(s)
            @pl.when((s >= 4) & (s < NB))
            def _(): pl.semaphore_signal(cred.at[1], 1, device_id={"dp": sib}, device_id_type=MESH)
        @pl.when(s < NB)
        def _():
            if comm:
                @pl.when(s >= RING)
                def _(): settle_gu(s - RING)
                @pl.when(s >= 1)
                def _(): d2d_gu(s - 1).wait_send()
            for half in (0, 1):
                g = lax.dot_general(a_s[:, HD * half:HD * (half + 1)], dgu_s[...], (((0,), (0,)), ((), ())), preferred_element_type=f32).astype(bf16)
                for pp in range(4):
                    k, q = (4 * half + pp) // 2, pp % 2
                    idx = jnp.where(core == q, s % RING, RING)
                    bgu[idx, k] = g[GRP * pp:GRP * (pp + 1), :]
            if comm:
                @pl.when(s >= RING)
                def _(): pl.semaphore_wait(cred.at[1], 1)
                d2d_gu(s).start()
        if comm:
            wait_sib_d(s)
            process_d(s)
            @pl.when((s >= 3) & (s < NB - 1))
            def _(): pl.semaphore_signal(cred.at[0], 1, device_id={"dp": sib}, device_id_type=MESH)
        if with_da:
            @pl.when(s < NB)
            def _():
                def dac(r, zz):
                    rows = pl.ds(pl.multiple_of(r * TC, TC), TC)
                    da_s[rows, :] += lax.dot_general(dgu_s[rows, :], w_s[w], (((1,), (1,)), ((), ())), preferred_element_type=f32)
                    return zz
                lax.fori_loop(0, T // TC, dac, 0)
                @pl.when(s == NB - 1)
                def _():
                    def nb(r, zz):
                        rows = pl.ds(pl.multiple_of(r * TC, TC), TC)
                        da = da_s[rows, :].astype(bf16).astype(f32)
                        wide = h_ref[rows, :].astype(f32)
                        scale = lax.rsqrt(jnp.mean(wide * wide, -1, keepdims=True) + 1e-6)
                        dscale = jnp.sum(da * wide, -1, keepdims=True)
                        c = dscale * (-1.0 / D) * (scale * scale * scale)
                        dho_ref[rows, :] = dh_ref[rows, :] + (da * scale + wide * c).astype(bf16)
                        return zz
                    lax.fori_loop(0, T // TC, nb, 0)
        return z
    lax.fori_loop(0, NB + 4 if comm else NB, step, 0)
    if comm:
        d2d_d(NB - 1).wait_send()
        d2d_gu(NB - 1).wait_send()
        for i in range(NB - RING, NB):
            settle_d(jnp.int32(i))
            settle_gu(jnp.int32(i))
    ss_ref[...] = jnp.full(ss_ref.shape, jnp.sum(ss_s[...]), f32)

def lcall(h, dh, wg, wu, wd, *, layer, with_da, comm=True):
    V = pl.BlockSpec(memory_space=pltpu.VMEM); A = pl.BlockSpec(memory_space=pl.ANY)
    S = jax.ShapeDtypeStruct
    outs = [S((NB, 2, GRP, 2 * BF), bf16), S((NB, HB, HD), bf16), S((8, 128), f32)]
    ospec = [A, A, V]
    if with_da:
        outs = [S((T, D), bf16)] + outs; ospec = [V] + ospec
    DMA = pltpu.SemaphoreType.DMA
    scratch = [pltpu.VMEM((T, D), bf16), pltpu.VMEM((2, D, 2 * BF), bf16), pltpu.VMEM((2, BF, D), bf16), pltpu.VMEM((T, BF), bf16), pltpu.VMEM((T, 2 * BF), bf16),
               pltpu.VMEM((RING + 1, 4, GRP, 2 * BF), bf16), pltpu.VMEM((RING + 1, 2, HB, HD), bf16), pltpu.VMEM((RING, 4, GRP, 2 * BF), bf16), pltpu.VMEM((RING, 2, HB, HD), bf16),
               pltpu.VMEM((2, NB, 2, GRP, 2 * BF), bf16), pltpu.VMEM((NB, 2, HB, HD), bf16), pltpu.VMEM((32, 2 * BF), f32)]
    if with_da: scratch.append(pltpu.VMEM((T, D), f32))
    scratch += [DMA((2, 3)), DMA((2, NB)), DMA((NB, 2)), DMA((RING, 2)), DMA((RING, 2)), DMA, DMA, DMA((RING,)), DMA((RING,)), DMA((RING,)), DMA((RING, 2)), pltpu.SemaphoreType.REGULAR((2,))]
    return pl.pallas_call(functools.partial(lkernel, layer=layer, with_da=with_da, comm=comm), out_shape=outs, in_specs=[V, V, A, A, A], out_specs=ospec,
        scratch_shapes=scratch, name=f"back{layer}",
        compiler_params=pltpu.CompilerParams(vmem_limit_bytes=67_000_000, **(dict(collective_id=layer, has_side_effects=True) if comm else {})))(h, dh, wg, wu, wd)


GR, DR = 32, 112
NG, ND = GRP // GR, DOWN // DR
MG = 4 * NG
NM = MG + 2 * ND
WS = 4
COUNT = 6 * D * F

def kc_kernel(gu1_ref, gu0_ref, d1_ref, d0_ref, ss_ref, wg, wu, wd, mg, mu, md, vg, vu, vd,
              nwg, nwu, nwd, nmg, nmu, nmd, nvg, nvu, nvd,
              ggu, gd, mb, vb, wb, mo, vo, wo, mbd, vbd, wbd, mod, vod, wod, ssr,
              lsem, rgu, rd, fgu, fd, psem, osem, wsem, rsem, relay_send, relay_sib, sibr, ssend, srecv):
    me = lax.axis_index("dp")
    chip = me // 2
    core = me % 2
    sib = me + 1 - 2 * core
    end = (chip == 0) | (chip == 3)
    guf, df = (gu0_ref, gu1_ref), (d0_ref, d1_ref)
    nw, w, m, v, nm, nv = (nwg, nwu, nwd), (wg, wu, wd), (mg, mu, md), (vg, vu, vd), (nmg, nmu, nmd), (nvg, nvu, nvd)

    def rdma(src, dst, ssem, rsem_, dev):
        return pltpu.make_async_remote_copy(src, dst, ssem, rsem_, device_id={"dp": dev}, device_id_type=MESH)

    kk = jnp.where(chip == 0, 0, 1)
    def own_g():
        out = []
        for l in (0, 1):
            out.append(pltpu.make_async_copy(guf[l].at[:, kk], ggu.at[l], lsem.at[2 * l]))
            out.append(pltpu.make_async_copy(df[l].at[pl.ds(pl.multiple_of(DOWN * (me % 4), 16), DOWN), :], gd.at[l, core], lsem.at[2 * l + 1]))
        return out
    @pl.when(end)
    def _():
        for c in own_g(): c.start()

    def parts(r):
        q = r // NG
        rd_ = r - MG
        return q // 2, q % 2, (r % NG) * GR, rd_ // ND, (rd_ % ND) * DR
    def each(r, fn):
        lg, mat, rg, ld, rdn = parts(r)
        for k in (0, 1):
            @pl.when((r < MG) & (mat == k))
            def _(): fn(k, lg, pl.multiple_of(rg, 16), GR)
        @pl.when(r >= MG)
        def _(): fn(2, ld, pl.multiple_of(rdn, 16), DR)

    def fetch(r):
        s = r % 2
        def fn(k, l, row, rows):
            def go():
                a, b, c = (mbd, vbd, wbd) if k == 2 else (mb, vb, wb)
                first = me * (DOWN if k == 2 else GRP) + row
                return (pltpu.make_async_copy(m[k].at[l, pl.ds(row, rows), :], a.at[s], psem.at[s, 0]),
                        pltpu.make_async_copy(v[k].at[l, pl.ds(row, rows), :], b.at[s], psem.at[s, 1]),
                        pltpu.make_async_copy(w[k].at[l, pl.ds(pl.multiple_of(first, 16), rows), :], c.at[s], psem.at[s, 2]))
            return go()
        return fn
    def start_fetch(r):
        def fn(*a):
            for c in fetch(r)(*a): c.start()
        each(r, fn)
    start_fetch(jnp.int32(0))

    bar = pltpu.get_barrier_semaphore()
    for t in range(1, 8):
        pl.semaphore_signal(bar, inc=1, device_id={"dp": lax.rem(me + t, 8)}, device_id_type=MESH)
    pl.semaphore_wait(bar, 7)

    slot = core + 2 * (me // 4)
    def ss_copy(t):
        return rdma(ss_ref, ssr.at[slot], ssend.at[t], srecv.at[slot], jnp.int32(t))
    @pl.when(end)
    def _():
        for t in range(8):
            @pl.when(me != t)
            def _(): ss_copy(t).start()

    def fwd_gu(r):
        k2 = 1 - kk
        out = []
        lg, mat, rg, _, _ = parts(r)
        rows = pl.ds(pl.multiple_of(rg, 16), GR)
        cols = pl.ds(pl.multiple_of(mat * BF, 128), BF)
        dev = jnp.where(chip == 0, me + 2, me - 2)
        for l in (0, 1):
            out.append((lg == l, rdma(guf[l].at[:, k2, rows, cols], ggu.at[l, :, rows, cols], fgu.at[r % 2], rgu.at[r], dev)))
        return out
    def fwd_d(r, q):
        _, _, _, ld, rdn = parts(r)
        dev = 4 * (me // 4) + q
        out = []
        for l in (0, 1):
            out.append(((ld == l) & (dev != me), rdma(df[l].at[pl.ds(pl.multiple_of(DOWN * q + rdn, 16), DR), :], gd.at[l, core, pl.ds(pl.multiple_of(rdn, 16), DR), :],
                        fd.at[q, r % 2], rd.at[r - MG, core], dev)))
        return out
    def forward(r):
        @pl.when(end & (r < MG))
        def _():
            for l, (cond, c) in enumerate(fwd_gu(r)):
                @pl.when(cond)
                def _(): c.start()
        @pl.when(end & (r >= MG) & (r < NM))
        def _():
            for q in range(4):
                for cond, c in fwd_d(r, q):
                    @pl.when(cond)
                    def _(): c.start()
    def forward_done(r):
        @pl.when(end & (r >= 0) & (r < MG))
        def _():
            for cond, c in fwd_gu(r):
                @pl.when(cond)
                def _(): c.wait_send()
        @pl.when(end & (r >= MG) & (r < NM))
        def _():
            for q in range(4):
                for cond, c in fwd_d(r, q):
                    @pl.when(cond)
                    def _(): c.wait_send()
    LEAD = 2
    for r in range(LEAD): forward(jnp.int32(r))

    @pl.when(end)
    def _():
        for c in own_g(): c.wait()
    total = jnp.zeros((8, 128), f32)
    for s, dev in enumerate((0, 1, 6, 7)):
        @pl.when(me != dev)
        def _(): rdma(ss_ref, ssr.at[s], ssend.at[0], srecv.at[s], jnp.int32(dev)).wait_recv()
        total += jnp.where(me == dev, ss_ref[...], ssr[s])
    factor = jnp.minimum(1.0, 0.5 * lax.rsqrt(total / COUNT + 1e-30))[0:1, 0:1]

    def adamw(wv, mv, vv, g):
        g = g.astype(f32) * factor
        mn = 0.9 * mv + 0.1 * g
        vn = 0.95 * vv + 0.05 * g * g
        wv = wv.astype(f32)
        return (wv - 0.02 * (mn * lax.rsqrt(vn + 1e-8) + 0.1 * wv)).astype(bf16), mn, vn

    def place(k, dev, l, row, rows):
        first = dev * (DOWN if k == 2 else GRP) + row
        return nw[k].at[l, pl.ds(pl.multiple_of(first, 16), rows), :]
    def own_w(r, k, l, row, rows):
        s = r % WS
        src = (wod if k == 2 else wo).at[s]
        dst = place(k, me, l, row, rows)
        return (lambda: pltpu.make_async_copy(src, dst, wsem.at[s, 0]),
                lambda: rdma(src, dst, wsem.at[s, 1], rsem.at[0, 0, r], me + 2),
                lambda: rdma(src, dst, wsem.at[s, 2], rsem.at[1, 0, r], me - 2),
                lambda: rdma(src, dst, wsem.at[s, 3], sibr.at[k], sib))
    def own_mv(r, k, l, row, rows):
        s = r % 2
        a, b = (mod, vod) if k == 2 else (mo, vo)
        return (pltpu.make_async_copy(a.at[s], nm[k].at[l, pl.ds(row, rows), :], osem.at[s, 0]),
                pltpu.make_async_copy(b.at[s], nv[k].at[l, pl.ds(row, rows), :], osem.at[s, 1]))
    def own_sent(r):
        def fn(*a):
            c, right, left, other = own_w(r, *a)
            c().wait()
            @pl.when(chip < 3)
            def _(): right().wait_send()
            @pl.when(chip > 0)
            def _(): left().wait_send()
            other().wait_send()
        each(r, fn)
    def own_mv_done(r):
        def fn(*a):
            for c in own_mv(r, *a): c.wait()
        each(r, fn)

    def own(r):
        s = r % 2
        s4 = r % WS
        @pl.when(r + 1 < NM)
        def _(): start_fetch(r + 1)
        forward_done(r + LEAD - 2)
        forward(r + LEAD)
        def fw(*a):
            for c in fetch(r)(*a): c.wait()
        each(r, fw)
        @pl.when(r >= WS)
        def _(): own_sent(r - WS)
        @pl.when(r >= 2)
        def _(): own_mv_done(r - 2)
        lg, mat, rg, ld, rdn = parts(r)
        @pl.when(r < MG)
        def _():
            @pl.when(~end)
            def _():
                rows = pl.ds(pl.multiple_of(rg, 16), GR); cols = pl.ds(pl.multiple_of(mat * BF, 128), BF)
                rdma(guf[0].at[:, 0, rows, cols], ggu.at[lg, :, rows, cols], fgu.at[0], rgu.at[r], me).wait_recv()
            def blk(t, z):
                b, hh = t // (GR // 16), t % (GR // 16)
                c = pl.ds(pl.multiple_of(b * BF, 128), BF)
                rr = pl.ds(pl.multiple_of(hh * 16, 16), 16)
                g = ggu[lg, b, pl.ds(pl.multiple_of(rg + hh * 16, 16), 16), pl.ds(pl.multiple_of(mat * BF, 128), BF)]
                a, bb, cc = adamw(wb[s, rr, c], mb[s, rr, c], vb[s, rr, c], g)
                wo[s4, rr, c] = a; mo[s, rr, c] = bb; vo[s, rr, c] = cc
                return z
            lax.fori_loop(0, NB * (GR // 16), blk, 0)
        @pl.when(r >= MG)
        def _():
            for h in (0, 1):
                @pl.when(~(end & (core == h)))
                def _():
                    rows = pl.ds(pl.multiple_of(rdn, 16), DR)
                    rdma(df[0].at[pl.ds(0, DR), :], gd.at[ld, h, rows, :], fd.at[0, 0], rd.at[r - MG, h], me).wait_recv()
            for h in (0, 1):
                def blk(t, z):
                    rr = pl.ds(pl.multiple_of(t * 16, 16), 16)
                    c = pl.ds(HD * h, HD)
                    g = gd[ld, h, pl.ds(pl.multiple_of(rdn + t * 16, 16), 16), :]
                    a, bb, cc = adamw(wbd[s, rr, c], mbd[s, rr, c], vbd[s, rr, c], g)
                    wod[s4, rr, c] = a; mod[s, rr, c] = bb; vod[s, rr, c] = cc
                    return z
                lax.fori_loop(0, DR // 16, blk, 0)
        def send(*a):
            c, right, left, other = own_w(r, *a)
            @pl.when(chip > 0)
            def _(): left().start()
            @pl.when(chip < 3)
            def _(): right().start()
            other().start()
            c().start()
            for c in own_mv(r, *a): c.start()
        each(r, send)

    def relay_copies(dr, dist, r, k, l, row, rows):
        dev = me + 2 * dist if dr else me - 2 * dist
        ref = place(k, dev, l, row, rows)
        to = me - 2 if dr else me + 2
        return (lambda: rdma(ref, ref, relay_send.at[dr, dist - 1], rsem.at[dr, dist, r], to),
                lambda: rdma(ref, ref, relay_sib.at[dr, dist - 1], sibr.at[k], sib),
                lambda: rdma(ref, ref, relay_send.at[dr, dist - 1], rsem.at[dr, dist - 1, r], to))
    def relay_sent(dr, dist, r, onward):
        def fn(*a):
            on, other, _ = relay_copies(dr, dist, r, *a)
            @pl.when(onward)
            def _(): on().wait_send()
            other().wait_send()
        each(r, fn)
    def relays(r, z):
        for dr in (0, 1):
            def one(dist, zz):
                rr = r - dist
                there = (chip + dist <= 3) if dr else (chip - dist >= 0)
                onward = (chip > 0) if dr else (chip < 3)
                @pl.when(there & (rr >= 0) & (rr < NM))
                def _():
                    @pl.when(rr >= 1)
                    def _(): relay_sent(dr, dist, rr - 1, onward)
                    def fn(*a):
                        on, other, came = relay_copies(dr, dist, rr, *a)
                        came().wait_recv()
                        @pl.when(onward)
                        def _(): on().start()
                        other().start()
                    each(rr, fn)
                    @pl.when(rr == NM - 1)
                    def _(): relay_sent(dr, dist, rr, onward)
                return zz
            lax.fori_loop(1, 4, one, 0)
    def rnd(r, z):
        @pl.when(r < NM)
        def _(): own(r)
        relays(r, z)
        return z
    lax.fori_loop(0, NM + 3, rnd, 0)
    for r in range(NM - WS, NM): own_sent(jnp.int32(r))
    for r in range(NM - 2, NM): own_mv_done(jnp.int32(r))
    for r in range(NM + LEAD - 2, NM): forward_done(jnp.int32(r))
    for k in range(3):
        rdma(nw[k].at[0], nw[k].at[0], wsem.at[0, 0], sibr.at[k], sib).wait_recv()
    @pl.when(end)
    def _():
        for t in range(8):
            @pl.when(me != t)
            def _(): ss_copy(t).wait_send()

def kcall(gu1, gu0, d1, d0, ss, ws, ms, vs):
    V = pl.BlockSpec(memory_space=pltpu.VMEM); A = pl.BlockSpec(memory_space=pl.ANY)
    S = jax.ShapeDtypeStruct
    DMA = pltpu.SemaphoreType.DMA
    outs = [S(w.shape, bf16) for w in ws] + [S(m.shape, f32) for m in ms] * 2
    VM = pltpu.VMEM
    scratch = [VM((2, NB, GRP, 2 * BF), bf16), VM((2, 2, DOWN, HD), bf16),
        VM((2, GR, F), f32), VM((2, GR, F), f32), VM((2, GR, F), bf16), VM((2, GR, F), f32), VM((2, GR, F), f32), VM((WS, GR, F), bf16),
        VM((2, DR, D), f32), VM((2, DR, D), f32), VM((2, DR, D), bf16), VM((2, DR, D), f32), VM((2, DR, D), f32), VM((WS, DR, D), bf16),
        VM((4, 8, 128), f32),
        DMA((4,)), DMA((MG,)), DMA((2 * ND, 2)), DMA((2,)), DMA((4, 2)), DMA((2, 3)), DMA((2, 2)), DMA((WS, 4)), DMA((2, 4, NM)), DMA((2, 3)), DMA((2, 3)), DMA((3,)), DMA((8,)), DMA((4,))]
    return pl.pallas_call(kc_kernel, out_shape=outs, in_specs=[A] * 4 + [V] + [A] * 9, out_specs=[A] * 9, scratch_shapes=scratch, name="gather",
        compiler_params=pltpu.CompilerParams(vmem_limit_bytes=40 << 20, collective_id=2, has_side_effects=True))(
        gu1, gu0, d1.reshape(F // 2, HD), d0.reshape(F // 2, HD), ss, *ws, *ms, *vs)


def solution(mesh):
    def body(x, dy, *arrays):
        weights, m, v = (arrays[i : i + 3] for i in (0, 3, 6))
        x, dy = x[0], dy[0]
        h = ka(x, *weights)
        dh, gu1, d1, ss1 = lcall(h, dy, *weights, layer=1, with_da=True)
        gu0, d0, ss0 = lcall(x, dh, *weights, layer=0, with_da=False)
        return tuple(kcall(gu1, gu0, d1, d0, ss1 + ss0, weights, m, v))

    shard = P(None, "dp", None)
    return jax.shard_map(
        body,
        mesh=mesh,
        in_specs=(P(("rep", "dp")),) * 2 + (P(),) * 3 + (shard,) * 6,
        out_specs=(P("rep"),) * 3 + (P("rep", "dp", None),) * 6,
        check_vma=False,
    )
```
